32 devices in a mesh: gx: 8 (over y, x, core), gy: 4 (over z).
Axes of the slice: x: 2, y: 2, z: 4, core: 2. Of those that a mesh axis runs over, the one named last changes fastest.
Arguments:
- fields: float32 [5, 128, 128, 128], P(None, 'gx', 'gy'), may hold values from -6 to 6
- patch_weight: bfloat16 [2560, 512], replicated, may hold values from -0.125 to 0.125
- trainer_of: int32 [2048, 1], P(('gx', 'gy')), may hold values from 0 to 31; in each aligned block of 64 rows (0 to 63, 64 to 127, ...) at most 4 rows name the same one
- lag_index: int32 [16, 16, 16], P('gx', 'gy'), may hold values from 0 to 1
- w_in: bfloat16 [32, 512, 2048], P(('gx', 'gy')), may hold values from -0.25 to 0.25
- b_in: float32 [32, 2048], P(('gx', 'gy')), may hold values from -3 to 3
- w_out: bfloat16 [32, 2048, 512], P(('gx', 'gy')), may hold values from -0.125 to 0.125
- b_out: float32 [32, 512], P(('gx', 'gy')), may hold values from -3 to 3
Outputs:
- new_fields: float32 [5, 128, 128, 128], P(None, 'gx', 'gy')
- patch_gradient: float32 [2560, 512], replicated
- w_in_gradient: float32 [32, 512, 2048], P(('gx', 'gy'))
- b_in_gradient: float32 [32, 2048], P(('gx', 'gy'))
- w_out_gradient: float32 [32, 2048, 512], P(('gx', 'gy'))
- b_out_gradient: float32 [32, 512], P(('gx', 'gy'))
The draws below stay inside these ranges and needn't reach their ends.
Inputs may be any that keep to these rules, and one draw needn't show every extreme that they name: `trainer_of`: among the 64 rows of one brick, no trainer is named more than 4 times.
All inputs are finite; a program needn't handle non-finite values.
Results may differ from the reference program's by a relative error of at most 0.0062.
Values may be sent and summed in bfloat16 or wider, within the bound.
A program may use at most 128 MiB of HBM per device.

```python
import math
import jax
import jax.numpy as jnp
import numpy as np
from jax import lax

FIELDS = 5
PATCH = 8
CX = 16
CY = 32
CZ = 128
STEPS = 3
EMBED = 512
HIDDEN_SIZE = 2048
BLOCK_ROWS = 2
FEAT = 2560
NX = 128
NY = 128
NBLOCK = 64
TRAINERS = 32
SLOTS = 4
ROWS = 4096
N_GX = 8
N_GY = 4
DEVICES = 32


def with_ends(result, key, low, top_value):
    place = [jax.random.randint(jax.random.fold_in(key, axis), (), 0, length) for axis, length in enumerate(result.shape)]
    main_axis = result.shape.index(max(result.shape))
    beside = place[:main_axis] + [(place[main_axis] + 1) % result.shape[main_axis]] + place[main_axis + 1:]
    return result.at[tuple(place)].set(low).at[tuple(beside)].set(top_value)


def levels(rng, dims, pieces, least, high):
    gain, own = 1.0, jax.random.fold_in(rng, 6)
    for dim, parts in pieces:
        heights = jnp.exp(jax.random.uniform(jax.random.fold_in(own, dim), (parts,), jnp.float32, least / len(pieces), high / len(pieces)))
        gain = gain * jnp.repeat(heights, dims[dim] // parts).reshape([-1 if axis == dim else 1 for axis in range(len(dims))])
    return gain


def shared_out(stream_key, own, number, rows, count, top, reach, lean):
    sequence = jax.random.permutation(stream_key, count)
    heavy_load, common = shares(count, rows * top, reach, lean, True), shares(count, rows * top, reach, lean, False)
    places = jnp.arange(count)

    def named(sizes, turn):
        used = int((sizes > 0).sum())
        fixed = max(1, used // 4)
        moved = fixed + (places - fixed + turn * (used - fixed)) % max(1, count - fixed)
        return jnp.zeros((count,), jnp.int32).at[sequence[jnp.where(places < fixed, places, moved)]].set(jnp.asarray(sizes, jnp.int32))

    sizes = jnp.where(number % 4 == 0, named(heavy_load, number // 4), named(common, number - number // 4 - 1))
    mixed = jax.random.permutation(jax.random.fold_in(own, 3), count)
    donor, sink = mixed[0:count // 2 * 2:2], mixed[1:count // 2 * 2:2]
    slack = jnp.minimum(sizes[donor] - 1, reach - sizes[sink]) // 2
    slack = jnp.where((donor == sequence[0]) | (sink == sequence[0]) | (sizes[sink] == 0), 0, jnp.maximum(slack, 0))
    moved = jax.random.randint(jax.random.fold_in(own, 4), (count // 2,), 0, 1 << 20) % (slack + 1)
    sizes = sizes.at[donor].add(-moved).at[sink].add(moved)
    members = jnp.searchsorted(jnp.cumsum(sizes), jnp.arange(rows * top), side="right").astype(jnp.int32)
    listing = members.reshape(top, rows).T
    listing = listing[jax.random.permutation(jax.random.fold_in(own, 1), rows)]
    turn = jax.random.randint(jax.random.fold_in(own, 2), (rows, 1), 0, top)
    return jnp.take_along_axis(listing, (jnp.arange(top)[None, :] + turn) % top, axis=1)


def shares(number_of, total, reach, lean, full):
    portions = [(1 << 20) // math.isqrt(rank ** lean) + 1 for rank in range(1, number_of + 1)]
    largest = reach if full else min(reach, max(-(-total // number_of), total * portions[0] // sum(portions)))
    least = 1 if total - largest >= number_of - 1 else 0
    counts, spare = [largest] + [least] * (number_of - 1), total - largest - least * (number_of - 1)
    while spare > 0:
        movable = [i for i in range(1, number_of) if counts[i] < largest] or [i for i in range(1, number_of) if counts[i] < reach]
        mass, remaining = sum([portions[i] for i in movable]), spare
        for i in movable:
            more = min(reach - counts[i], max(1, remaining * portions[i] // mass), spare)
            counts[i] = counts[i] + more
            spare = spare - more
    return np.array(counts)


def centred(own_key, dims, deviation, most, shards=(), kind=jnp.bfloat16):
    entries = jax.random.normal(own_key, dims, jnp.float32) * deviation
    if len(shards) > 0:
        entries = levels(own_key, dims, shards, -0.22, 0.18) * entries
    return jnp.clip(entries, min=-most, max=most).astype(kind)


def setup_inputs(seed: int = 0) -> dict:
    splits = jax.random.split(jax.random.key(seed), 9)
    fields = centred(splits[0], (FIELDS, NX, NY, CZ), 1.0, 6.0, ((1, 8), (2, 4)), jnp.float32)
    patch_weight = centred(splits[1], (FEAT, EMBED), FEAT ** -0.5, 0.125)
    trainer_of_keys = jax.random.split(jax.random.fold_in(splits[2], 1), (TRAINERS * NBLOCK) // NBLOCK)
    trainer_of_turns = jax.random.permutation(jax.random.fold_in(splits[2], 3), (TRAINERS * NBLOCK) // NBLOCK)
    trainer_of = jax.vmap(lambda own, number: shared_out(jax.random.fold_in(splits[2], 2), own, number, NBLOCK, TRAINERS, 1, SLOTS, 2))(trainer_of_keys, trainer_of_turns).reshape((TRAINERS * NBLOCK, 1))
    lag_index = with_ends(jax.random.randint(splits[3], (NX // PATCH, NY // PATCH, CZ // PATCH), 0, STEPS - 1), jax.random.fold_in(splits[3], 1), 0, (STEPS - 1) - 1).astype(jnp.int32)
    w_in = centred(splits[4], (TRAINERS, EMBED, HIDDEN_SIZE), EMBED ** -0.5, 0.25, ((0, 32),))
    b_in = centred(splits[5], (TRAINERS, HIDDEN_SIZE), 0.5, 3.0, ((0, 32),), jnp.float32)
    w_out = centred(splits[6], (TRAINERS, HIDDEN_SIZE, EMBED), HIDDEN_SIZE ** -0.5, 0.125, ((0, 32),))
    b_out = centred(splits[7], (TRAINERS, EMBED), 0.5, 3.0, ((0, 32),), jnp.float32)
    return {"fields": fields, "patch_weight": patch_weight, "trainer_of": trainer_of, "lag_index": lag_index, "w_in": w_in, "b_in": b_in, "w_out": w_out, "b_out": b_out}


time_step = 0.2
viscosity = 0.5
drift_x = 0.6
drift_y = -0.4
drift_z = 0.3
error_weight = 0.0625


def shifted(padded, dimension, offset):
    window = [slice(None)]
    for other in (1, 2, 3):
        window.append(slice(2, padded.shape[other] - 2))
    window[dimension] = slice(2 + offset, padded.shape[dimension] - 2 + offset)
    return padded[tuple(window)]


def tendency(padded):
    gradients = []
    laplacian = 0.0
    for dimension in (1, 2, 3):
        back_two = shifted(padded, dimension, -2)
        back_one = shifted(padded, dimension, -1)
        middle = shifted(padded, dimension, 0)
        ahead_one = shifted(padded, dimension, 1)
        ahead_two = shifted(padded, dimension, 2)
        gradients.append((back_two - 8.0 * back_one + 8.0 * ahead_one - ahead_two) / 12.0)
        laplacian = laplacian + (-back_two + 16.0 * back_one - 30.0 * middle + 16.0 * ahead_one - ahead_two) / 12.0
    carried = drift_x * gradients[0] + drift_y * gradients[1] + drift_z * gradients[2]
    divergence = gradients[0][1] + gradients[1][2] + gradients[2][3]
    acoustic = jnp.stack([divergence, gradients[0][4], gradients[1][4], gradients[2][4], divergence])
    return viscosity * laplacian - carried - acoustic


def contract_rows(left, right):
    return lax.dot_general(left, right, (((0,), (0,)), ((), ())), preferred_element_type=jnp.float32)


def contract_cols(left, right):
    return lax.dot_general(left, right, (((1,), (1,)), ((), ())), preferred_element_type=jnp.float32)


def trainer_step(source, target, valid, w_first, b_first, w_second, b_second):
    pre = jnp.dot(source, w_first, preferred_element_type=jnp.float32) + b_first
    hidden = jax.nn.silu(pre).astype(jnp.bfloat16)
    predict = jnp.dot(hidden, w_second, preferred_element_type=jnp.float32) + b_second
    error = (error_weight * (predict - target.astype(jnp.float32)) * valid).astype(jnp.bfloat16)
    b_second_grad = jnp.sum(error.astype(jnp.float32), axis=0)
    w_second_grad = contract_rows(hidden, error)
    back = contract_cols(error, w_second)
    sigma = jax.nn.sigmoid(pre)
    pre_grad = (back * sigma * (1.0 + pre * (1.0 - sigma))).astype(jnp.bfloat16)
    b_first_grad = jnp.sum(pre_grad.astype(jnp.float32), axis=0)
    w_first_grad = contract_rows(source, pre_grad)
    source_grad = contract_cols(pre_grad, w_first).astype(jnp.bfloat16)
    return source_grad, w_first_grad, b_first_grad, w_second_grad, b_second_grad


def patchify(state):
    shaped = state.reshape(FIELDS, N_GX, CX // PATCH, PATCH, N_GY, CY // PATCH, PATCH, CZ // PATCH, PATCH)
    return shaped.transpose(1, 4, 2, 5, 7, 0, 3, 6, 8).reshape(ROWS, FEAT)


def one_trainer(operands):
    return trainer_step(*operands)


def reference(fields, patch_weight, trainer_of, lag_index, w_in, b_in, w_out, b_out):
    current = fields
    states = []
    for counter in range(STEPS):
        padded = jnp.pad(current, ((0, 0), (2, 2), (2, 2), (2, 2)))
        current = current + time_step * tendency(padded)
        states.append(current)
    lag_rows = lag_index.reshape(N_GX, CX // PATCH, N_GY, CY // PATCH, CZ // PATCH)
    lag_rows = lag_rows.transpose(0, 2, 1, 3, 4).reshape(ROWS, 1)
    picked = patchify(states[0].astype(jnp.bfloat16))
    for counter in range(1, STEPS - 1):
        picked = jnp.where(lag_rows == counter, patchify(states[counter].astype(jnp.bfloat16)), picked)
    source = jnp.dot(picked, patch_weight, preferred_element_type=jnp.float32).astype(jnp.bfloat16)
    target = jnp.dot(patchify(current.astype(jnp.bfloat16)), patch_weight,
                     preferred_element_type=jnp.float32).astype(jnp.bfloat16)
    owners = trainer_of[:, 0].reshape(DEVICES, NBLOCK)
    onehot = (owners[:, :, None] == jnp.arange(TRAINERS, dtype=jnp.int32)[None, None, :]).astype(jnp.int32)
    within_rank = jnp.sum((jnp.cumsum(onehot, axis=1) - onehot) * onehot, axis=2)
    senders = jnp.arange(DEVICES, dtype=jnp.int32)[:, None]
    slot_block = (owners * DEVICES + senders) * SLOTS + within_rank
    slot_row = (slot_block[:, :, None] * BLOCK_ROWS + jnp.arange(BLOCK_ROWS, dtype=jnp.int32)[None, None, :])
    slot_row = slot_row.reshape(ROWS).astype(jnp.int32)
    capacity = TRAINERS * DEVICES * SLOTS * BLOCK_ROWS
    per_trainer = DEVICES * SLOTS * BLOCK_ROWS
    packed_source = jnp.zeros((capacity, EMBED), source.dtype).at[slot_row].set(source)
    packed_target = jnp.zeros((capacity, EMBED), target.dtype).at[slot_row].set(target)
    packed_valid = jnp.zeros((capacity, 1), jnp.float32).at[slot_row].set(1.0)
    results = lax.map(one_trainer, (packed_source.reshape(TRAINERS, per_trainer, EMBED),
                                    packed_target.reshape(TRAINERS, per_trainer, EMBED),
                                    packed_valid.reshape(TRAINERS, per_trainer, 1),
                                    w_in, b_in, w_out, b_out))
    source_grad = results[0].reshape(capacity, EMBED)[slot_row]
    patch_gradient = contract_rows(picked, source_grad)
    return current, patch_gradient, results[1], results[2], results[3], results[4]
```

```python
import jax
import jax.numpy as jnp
from jax import lax
from jax.experimental import pallas as pl
from jax.experimental.pallas import tpu as pltpu
from jax.sharding import PartitionSpec as P

FIELDS = 5
PATCH = 8
STEPS = 3
EMBED = 512
BLOCK_ROWS = 2


time_step = 0.2
viscosity = 0.5
drift_x = 0.6
drift_y = -0.4
drift_z = 0.3
error_weight = 0.0625


def with_halo(cells, sides, width):
    for axis, dim in sides:
        count = lax.axis_size(axis)
        ends = count - 1
        head = lax.slice_in_dim(cells, 0, width, axis=dim)
        tail = lax.slice_in_dim(cells, cells.shape[dim] - width, cells.shape[dim], axis=dim)
        cells = jnp.concatenate(
            [
                lax.ppermute(tail, axis, [(i, (i + 1) % count) for i in range(ends)]),
                cells,
                lax.ppermute(head, axis, [((i + 1) % count, i) for i in range(ends)]),
            ],
            axis=dim,
        )
    return cells


def shifted(padded, dimension, offset):
    window = [slice(None)]
    for other in (1, 2, 3):
        window.append(slice(2, padded.shape[other] - 2))
    window[dimension] = slice(2 + offset, padded.shape[dimension] - 2 + offset)
    return padded[tuple(window)]


def tendency(padded):
    gradients = []
    laplacian = 0.0
    for dimension in (1, 2, 3):
        back_two = shifted(padded, dimension, -2)
        back_one = shifted(padded, dimension, -1)
        middle = shifted(padded, dimension, 0)
        ahead_one = shifted(padded, dimension, 1)
        ahead_two = shifted(padded, dimension, 2)
        gradients.append((back_two - 8.0 * back_one + 8.0 * ahead_one - ahead_two) / 12.0)
        laplacian = (
            laplacian
            + (-back_two + 16.0 * back_one - 30.0 * middle + 16.0 * ahead_one - ahead_two) / 12.0
        )
    carried = drift_x * gradients[0] + drift_y * gradients[1] + drift_z * gradients[2]
    divergence = gradients[0][1] + gradients[1][2] + gradients[2][3]
    acoustic = jnp.stack(
        [divergence, gradients[0][4], gradients[1][4], gradients[2][4], divergence]
    )
    return viscosity * laplacian - carried - acoustic


def contract_rows(left, right):
    return lax.dot_general(
        left, right, (((0,), (0,)), ((), ())), preferred_element_type=jnp.float32
    )


def contract_cols(left, right):
    return lax.dot_general(
        left, right, (((1,), (1,)), ((), ())), preferred_element_type=jnp.float32
    )


def trainer_step(source, target, valid, w_first, b_first, w_second, b_second):
    pre = jnp.dot(source, w_first, preferred_element_type=jnp.float32) + b_first
    hidden = jax.nn.silu(pre).astype(jnp.bfloat16)
    predict = jnp.dot(hidden, w_second, preferred_element_type=jnp.float32) + b_second
    error = (error_weight * (predict - target.astype(jnp.float32)) * valid).astype(jnp.bfloat16)
    b_second_grad = jnp.sum(error.astype(jnp.float32), axis=0)
    w_second_grad = contract_rows(hidden, error)
    back = contract_cols(error, w_second)
    sigma = jax.nn.sigmoid(pre)
    pre_grad = (back * sigma * (1.0 + pre * (1.0 - sigma))).astype(jnp.bfloat16)
    b_first_grad = jnp.sum(pre_grad.astype(jnp.float32), axis=0)
    w_first_grad = contract_rows(source, pre_grad)
    source_grad = contract_cols(pre_grad, w_first).astype(jnp.bfloat16)
    return (source_grad, w_first_grad, b_first_grad, w_second_grad, b_second_grad)


def patch_kernel(cells_ref, rows_ref, *turned):
    count, inner, lanes = rows_ref.shape[0], cells_ref.shape[1], turned[0].shape[1]
    for part, piece in enumerate(turned):
        cells = cells_ref[0, part * lanes : min(inner, (part + 1) * lanes), :]
        if cells.shape[0] < lanes:
            cells = jnp.concatenate(
                [cells, jnp.zeros((lanes - cells.shape[0], cells.shape[1]), cells.dtype)], axis=0
            )
        piece[...] = cells.T
    parts = []
    for offset in range(PATCH):
        for part, piece in enumerate(turned):
            rows = piece[pl.ds(offset, count, stride=PATCH), :]
            parts.append(rows[:, : min(lanes, inner - part * lanes)])
    rows_ref[...] = jnp.concatenate(parts, axis=1).astype(rows_ref.dtype)


def patchify(state):
    width_x, width_y, width_z = (state.shape[1], state.shape[2], state.shape[3])
    shaped = state.reshape(FIELDS, width_x // PATCH, PATCH, width_y // PATCH, PATCH, width_z)
    cells = shaped.transpose(1, 3, 0, 2, 4, 5).reshape(-1, FIELDS * PATCH * PATCH, width_z)
    columns, inner = cells.shape[0], cells.shape[1]
    count = width_z // PATCH
    return pl.pallas_call(
        patch_kernel,
        grid=(columns,),
        out_shape=jax.ShapeDtypeStruct((columns * count, inner * PATCH), jnp.bfloat16),
        in_specs=[pl.BlockSpec((1, inner, width_z), lambda i: (i, 0, 0))],
        out_specs=pl.BlockSpec((count, inner * PATCH), lambda i: (i, 0)),
        scratch_shapes=[pltpu.VMEM((width_z, 128), jnp.float32)] * pl.cdiv(inner, 128),
        cost_estimate=pl.CostEstimate(
            flops=8 * cells.size, bytes_accessed=6 * cells.size, transcendentals=0
        ),
    )(cells)


def pick(first, second, lag_index):
    count_x, count_y, count_z = lag_index.shape
    lag = jnp.repeat(lag_index, PATCH, axis=2)
    lag = lag.reshape(1, count_x, 1, count_y, 1, count_z * PATCH)
    shape = (FIELDS, count_x, PATCH, count_y, PATCH, count_z * PATCH)
    return jnp.where(lag == 1, second.reshape(shape), first.reshape(shape)).reshape(first.shape)


def pad_third(current):
    return jnp.pad(current, ((0, 0), (0, 0), (0, 0), (2, 2)))


def advance(fields):
    states = []
    current = fields
    for counter in range(STEPS):
        padded = with_halo(current, (("gx", 1), ("gy", 2)), 2)
        current = current + time_step * tendency(pad_third(padded))
        states.append(current)
    return states


def per_device(fields, patch_weight, trainer_of, lag_index, w_in, b_in, w_out, b_out):
    states = advance(fields)
    devices = lax.axis_size("gx") * lax.axis_size("gy")
    picked = patchify(pick(states[0], states[1], lag_index))
    embed = patch_weight.shape[1]
    weight = patch_weight.reshape(-1, PATCH, embed).transpose(1, 0, 2).reshape(-1, embed)
    target = jnp.dot(
        patchify(states[-1]), weight, preferred_element_type=jnp.float32
    ).astype(jnp.bfloat16)
    patch_count = picked.shape[0]
    block_count = patch_count // BLOCK_ROWS
    slot_count = max(2, 2 * block_count // devices)
    owners = trainer_of[:, 0]
    onehot = (owners[:, None] == jnp.arange(devices, dtype=jnp.int32)[None, :]).astype(jnp.int32)
    within_rank = jnp.sum((jnp.cumsum(onehot, axis=0) - onehot) * onehot, axis=1)
    block_slot = owners * slot_count + within_rank

    patch_slot = jnp.repeat(block_slot, BLOCK_ROWS) * BLOCK_ROWS
    patch_slot = patch_slot + jnp.arange(patch_count, dtype=jnp.int32) % BLOCK_ROWS
    slot_rows = slot_count * BLOCK_ROWS
    place = (
        jnp.arange(devices * slot_rows, dtype=jnp.int32)[:, None] == patch_slot[None, :]
    ).astype(jnp.bfloat16)

    def exchange(rows):
        packed = jnp.dot(place, rows, preferred_element_type=jnp.float32).astype(jnp.bfloat16)
        packed = packed.reshape(devices, slot_rows, rows.shape[1])
        got = lax.all_to_all(packed, ("gx", "gy"), split_axis=0, concat_axis=0, tiled=True)
        return got.reshape(devices * slot_rows, rows.shape[1])

    flat_patches = exchange(picked)
    got_target = exchange(jnp.concatenate([target, jnp.ones((patch_count, 128), jnp.bfloat16)], 1))
    source = jnp.dot(flat_patches, weight, preferred_element_type=jnp.float32).astype(
        jnp.bfloat16
    )
    valid_rows = got_target[:, embed : embed + 1].astype(jnp.float32)
    results = trainer_step(
        source, got_target[:, :embed], valid_rows, w_in[0], b_in[0], w_out[0], b_out[0]
    )
    partial_value = contract_rows(flat_patches, results[0])
    share = lax.psum_scatter(partial_value, ("gx", "gy"), scatter_dimension=0, tiled=True)
    summed = lax.all_gather(share.astype(jnp.bfloat16), ("gx", "gy"), axis=0, tiled=True)
    summed = summed.reshape(PATCH, -1, embed).transpose(1, 0, 2).reshape(-1, embed)
    patch_gradient = summed.astype(jnp.float32)
    return (
        states[-1],
        patch_gradient,
        results[1][None],
        results[2][None],
        results[3][None],
        results[4][None],
    )


def solution(mesh):
    in_specs = (
        P(None, "gx", "gy", None),
        P(),
        P(("gx", "gy"), None),
        P("gx", "gy", None),
        P(("gx", "gy"), None, None),
        P(("gx", "gy"), None),
        P(("gx", "gy"), None, None),
        P(("gx", "gy"), None),
    )
    out_specs = (
        P(None, "gx", "gy", None),
        P(),
        P(("gx", "gy"), None, None),
        P(("gx", "gy"), None),
        P(("gx", "gy"), None, None),
        P(("gx", "gy"), None),
    )
    return jax.shard_map(
        per_device, mesh=mesh, in_specs=in_specs, out_specs=out_specs, check_vma=False
    )
```
